32 devices in a mesh: agent: 2 (over x), row: 4 (over z), col: 4 (over y, core).
Axes of the slice: x: 2, y: 2, z: 4, core: 2. Of those that a mesh axis runs over, the one named last changes fastest.
Arguments:
- probe_field: float32 [2, 256, 256], replicated, may hold values from -4.2 to 4.2
- offsets: int32 [2, 16, 8], P(None, ('agent', 'row'), 'col'), may hold values from -32 to 32
- amplitudes: float32 [16, 8, 256, 256], P(('agent', 'row'), 'col'), may hold values from 0.2 to 2
- data_state: float32 [2, 1024, 512], P(None, ('agent', 'row'), 'col'), may hold values from -4.2 to 4.2
- prior_state: float32 [2, 1024, 512], P(None, ('agent', 'row', 'col')), may hold values from -4.2 to 4.2
- first_weights: bfloat16 [3, 32, 6], replicated, may hold values from -2 to 2
- middle_weights: bfloat16 [4, 3, 32, 96], replicated, may hold values from -0.5 to 0.5
- last_weights: bfloat16 [3, 2, 96], replicated, may hold values from -0.375 to 0.375
Outputs:
- data_next: float32 [2, 1024, 512], P(None, ('agent', 'row'), 'col')
- prior_next: float32 [2, 1024, 512], P(None, ('agent', 'row', 'col'))
The draws below stay inside these ranges and needn't reach their ends.
All inputs are finite; a program needn't handle non-finite values.
Results may differ from the reference program's by a relative error of at most 0.0073.
Values may be sent and summed in bfloat16 or wider, within the bound.
No kernel may reach another device: no remote copies, remote signals or barrier semaphores. Data moves between devices by JAX's collectives and lax.ppermute only.
A program may use at most 64 MiB of HBM per device.

```python
import math
import jax
import jax.numpy as jnp
from jax import lax

TILE_ROWS = 128
PROBE = 256
STEP = 64
JITTER = 32
CH = 32
LAYERS = 6
HALO = 128
HEIGHT = 1024
WIDTH = 512
POS_ROWS = 16
POS_COLS = 8


def plant(entries, key, least, high):
    longest = entries.shape.index(max(entries.shape))
    spots = []
    for shift in (0, 1):
        where = [jax.random.randint(jax.random.fold_in(key, axis), (), 0, length) for axis, length in enumerate(entries.shape)]
        where[longest] = (where[longest] + shift) % entries.shape[longest]
        spots.append(tuple(where))
    return entries.at[spots[0]].set(least).at[spots[1]].set(high)


def level_of(own_key, dims, cuts, smallest, high):
    def one(axis_at, shards_of):
        draws = jax.random.uniform(jax.random.fold_in(jax.random.fold_in(own_key, 6), axis_at), (shards_of,), jnp.float32, smallest / len(cuts), high / len(cuts))
        return jnp.repeat(jnp.exp(draws), dims[axis_at] // shards_of).reshape((-1,) + (1,) * (len(dims) - axis_at - 1))

    loudness = one(*cuts[0])
    for cut in cuts[1:]:
        loudness = loudness * one(*cut)
    return loudness


def gaussian(rng, dims, width, reach, shards=(), kind=jnp.bfloat16):
    values = width * jax.random.normal(rng, dims, jnp.float32)
    if shards:
        values = values * level_of(rng, dims, shards, -0.22, 0.18)
    return jnp.clip(values, -reach, reach).astype(kind)


def setup_inputs(seed: int = 0) -> dict:
    key_of = jax.random.split(jax.random.key(seed), 9)
    probe_field = gaussian(key_of[0], (2, PROBE, PROBE), 0.7, 4.2, (), jnp.float32)
    offsets = plant(jax.random.randint(key_of[1], (2, POS_ROWS, POS_COLS), 0 - JITTER, JITTER + 1), jax.random.fold_in(key_of[1], 1), 0 - JITTER, JITTER).astype(jnp.int32)
    amplitudes = jnp.clip(0.2 + 1.8 * jax.random.uniform(key_of[2], (POS_ROWS, POS_COLS, PROBE, PROBE), jnp.float32) ** level_of(key_of[2], (POS_ROWS, POS_COLS, PROBE, PROBE), ((0, 8), (1, 4)), -0.2, 0.2), 0.2, 2.0)
    data_state = gaussian(key_of[3], (2, HEIGHT, WIDTH), 0.7, 4.2, ((1, 8), (2, 4)), jnp.float32)
    prior_state = gaussian(key_of[4], (2, HEIGHT, WIDTH), 0.7, 4.2, ((1, 32),), jnp.float32)
    first_weights = gaussian(key_of[5], (3, CH, 6), 9 ** -0.5, 2.0)
    middle_weights = gaussian(key_of[6], (LAYERS - 2, 3, CH, 3 * CH), (9 * CH // 2) ** -0.5, 0.5)
    last_weights = gaussian(key_of[7], (3, 2, 3 * CH), (9 * CH) ** -0.5, 0.375)
    return {"probe_field": probe_field, "offsets": offsets, "amplitudes": amplitudes, "data_state": data_state, "prior_state": prior_state, "first_weights": first_weights, "middle_weights": middle_weights, "last_weights": last_weights}


MAGNITUDE_FLOOR = 0.5
DATA_STEP = 0.125
DATA_WEIGHT = 0.6
RELAXATION = 0.5

def as_index(value):
    return jnp.asarray(value).astype(jnp.int32)

def dft_tables():
    numbers = jnp.arange(PROBE, dtype=jnp.int32)
    product = numbers[:, None] * numbers[None, :] % PROBE
    angles = product.astype(jnp.float32) * (2.0 * math.pi / PROBE)
    scaling = 1.0 / math.sqrt(PROBE)
    return ((jnp.cos(angles) * scaling).astype(jnp.bfloat16), (-jnp.sin(angles) * scaling).astype(jnp.bfloat16))

def right_product(left_real, left_imag, table_real, table_imag):
    joined = jnp.concatenate([left_real, left_imag], axis=-1).astype(jnp.float32)
    table = jnp.concatenate([jnp.concatenate([table_real, table_imag], axis=1), jnp.concatenate([-table_imag, table_real], axis=1)], axis=0).astype(jnp.float32)
    output = jnp.einsum('bjk,kw->bjw', joined, table)
    midpoint = left_real.shape[-1]
    return (output[..., :midpoint], output[..., midpoint:])

def left_product(table_real, table_imag, right_real, right_imag):
    stacked = jnp.concatenate([table_real, table_imag], axis=0).astype(jnp.float32)
    first = jnp.einsum('jk,bkw->bjw', stacked, right_real.astype(jnp.float32))
    second = jnp.einsum('jk,bkw->bjw', stacked, right_imag.astype(jnp.float32))
    midpoint = table_real.shape[0]
    return (first[:, :midpoint] - second[:, midpoint:], first[:, midpoint:] + second[:, :midpoint])

def position_terms(patches, measured, probe_field, table_real, table_imag):
    probe_real = probe_field[0]
    probe_imag = probe_field[1]
    object_real = patches[:, 0]
    object_imag = patches[:, 1]
    exit_real = (probe_real * object_real - probe_imag * object_imag).astype(jnp.bfloat16)
    exit_imag = (probe_real * object_imag + probe_imag * object_real).astype(jnp.bfloat16)
    half_real, half_imag = right_product(exit_real, exit_imag, table_real, table_imag)
    wave_real, wave_imag = left_product(table_real, table_imag, half_real.astype(jnp.bfloat16), half_imag.astype(jnp.bfloat16))
    magnitude = jnp.sqrt(wave_real * wave_real + wave_imag * wave_imag)
    retained = 1.0 - measured / jnp.maximum(magnitude, MAGNITUDE_FLOOR)
    resid_real = (wave_real * retained).astype(jnp.bfloat16)
    resid_imag = (wave_imag * retained).astype(jnp.bfloat16)
    back_real, back_imag = right_product(resid_real, resid_imag, table_real, -table_imag)
    field_real, field_imag = left_product(table_real, -table_imag, back_real.astype(jnp.bfloat16), back_imag.astype(jnp.bfloat16))
    contrib_real = probe_real * field_real + probe_imag * field_imag
    contrib_imag = probe_real * field_imag - probe_imag * field_real
    return jnp.stack([contrib_real, contrib_imag], axis=1)

def convolve(current, weight):
    row_count = current.shape[1] - 2
    col_count = current.shape[2]
    widened = jnp.pad(current, ((0, 0), (0, 0), (1, 1)))
    summed = None
    for shift_row in range(3):
        stacked = jnp.concatenate([widened[:, shift_row:shift_row + row_count, shift_col:shift_col + col_count] for shift_col in range(3)], axis=0)
        contribution = jnp.einsum('ok,krw->orw', weight[shift_row].astype(jnp.float32), stacked.astype(jnp.float32))
        summed = contribution if summed is None else summed + contribution
    return summed

def denoise_rows(current, first_row, height, weights):
    output = None
    for depth in range(LAYERS):
        output = convolve(current, weights[depth])
        first_row = first_row + 1
        if depth < LAYERS - 1:
            row_ids = first_row + jnp.arange(output.shape[1], dtype=jnp.int32)
            inside = (row_ids >= 0) & (row_ids < height)
            current = jnp.where(inside[None, :, None], jax.nn.relu(output), 0.0).astype(jnp.bfloat16)
    return output

def reference(probe_field, offsets, amplitudes, data_state, prior_state, first_weights, middle_weights, last_weights):
    table_real, table_imag = dft_tables()
    padded = jnp.pad(data_state, ((0, 0), (HALO, HALO), (HALO, HALO)))
    col_base = jnp.arange(POS_COLS, dtype=jnp.int32) * STEP + JITTER
    anchor_zero = as_index(0)

    def row_pass(buffer, inputs):
        number, shifts, measured = inputs
        upper_edges = as_index(number * STEP + JITTER + shifts[0])
        left_edges = as_index(col_base + shifts[1])
        patches = jax.vmap(lambda upper_edge, left_edge: lax.dynamic_slice(padded, (anchor_zero, as_index(upper_edge), as_index(left_edge)), (2, PROBE, PROBE)))(upper_edges, left_edges)
        contributions = position_terms(patches, measured, probe_field, table_real, table_imag)

        def scatter_one(position, accumulator):
            upper_edge = as_index(upper_edges[position])
            left_edge = as_index(left_edges[position])
            current = lax.dynamic_slice(accumulator, (anchor_zero, upper_edge, left_edge), (2, PROBE, PROBE))
            return lax.dynamic_update_slice(accumulator, current + contributions[position], (anchor_zero, upper_edge, left_edge))
        return (lax.fori_loop(0, POS_COLS, scatter_one, buffer), None)
    scanned = lax.scan(row_pass, jnp.zeros(padded.shape, jnp.float32), (jnp.arange(POS_ROWS, dtype=jnp.int32), jnp.moveaxis(offsets, 1, 0).astype(jnp.int32), amplitudes))
    gradient = scanned[0][:, HALO:HALO + HEIGHT, HALO:HALO + WIDTH]
    data_update = data_state - DATA_STEP * gradient
    data_reflect = 2.0 * data_update - data_state
    weights = [first_weights] + [middle_weights[number] for number in range(LAYERS - 2)] + [last_weights]
    inputs = jnp.pad(prior_state.astype(jnp.bfloat16), ((0, 0), (LAYERS, LAYERS), (0, 0)))

    def block_pass(number):
        anchor = as_index(number * TILE_ROWS)
        window = lax.dynamic_slice(inputs, (anchor_zero, anchor, anchor_zero), (2, TILE_ROWS + 2 * LAYERS, WIDTH))
        return denoise_rows(window, anchor - LAYERS, HEIGHT, weights)
    blocks = lax.map(block_pass, jnp.arange(HEIGHT // TILE_ROWS, dtype=jnp.int32))
    noise = jnp.moveaxis(blocks, 0, 1).reshape(2, HEIGHT, WIDTH)
    prior_update = prior_state - noise
    prior_reflect = 2.0 * prior_update - prior_state
    consensus = DATA_WEIGHT * data_reflect + (1.0 - DATA_WEIGHT) * prior_reflect
    data_next = (1.0 - RELAXATION) * data_state + RELAXATION * (2.0 * consensus - data_reflect)
    prior_next = (1.0 - RELAXATION) * prior_state + RELAXATION * (2.0 * consensus - prior_reflect)
    return (data_next, prior_next)
```

```python
import functools
import math

import jax
import jax.numpy as jnp
import numpy as np
from jax import lax
from jax.experimental import pallas as pl
from jax.experimental.pallas import tpu as pltpu
from jax.sharding import PartitionSpec as P

PROBE = 256
STEP = 64
JITTER = 32
LAYERS = 6
HALO = 128
EDGE = 8
BAND = 4
LAST_BAND = 16

MAGNITUDE_FLOOR = 0.5
DATA_STEP = 0.125
DATA_WEIGHT = 0.6
RELAXATION = 0.5

ROWS = ("agent", "row")
STRIPS = ("agent", "row", "col")

VMEM = pl.BlockSpec(memory_space=pltpu.VMEM)
SMEM = pl.BlockSpec(memory_space=pltpu.SMEM)
BF16 = jnp.bfloat16
F32 = jnp.float32


def params(mib=48):
    return pltpu.CompilerParams(vmem_limit_bytes=mib * 1024 * 1024)


def dft_blocks():
    numbers = np.arange(PROBE)
    angles = (numbers[:, None] * numbers[None, :] % PROBE) * (2.0 * math.pi / PROBE)
    real = np.cos(angles) / math.sqrt(PROBE)
    imag = -np.sin(angles) / math.sqrt(PROBE)
    forward = np.block([[real, imag], [-imag, real]])
    return jnp.asarray(forward, BF16), jnp.asarray(forward.T.copy(), BF16)


def ring(value, axes, shift):
    count = lax.axis_size(axes)
    return lax.ppermute(value, axes, [(i, (i + shift) % count) for i in range(count)])


def band_kernel(strip, first_ref, middle_ref, last_ref, t1_ref, tm_ref, t6_ref, lane_ref, few_ref, line_ref):
    channels = middle_ref.shape[2]
    wide = middle_ref.shape[3]
    rows_in = strip + 2 * EDGE
    rows_out = strip + 2 * (LAYERS - 1)
    lane_ref[...] = jnp.zeros_like(lane_ref)

    def widened(piece, lanes):
        height = piece.shape[0]
        lane_ref[:height, :wide] = piece
        value = lane_ref[:height, :]
        return jnp.concatenate([value, jnp.zeros((height, lanes - 128), F32)], axis=1)

    span = tm_ref.shape[2]
    lanes = -(-span // 128) * 128
    for layer in range(middle_ref.shape[0]):
        base = None
        for a in range(3):
            piece = widened(middle_ref[layer, a].astype(F32), lanes)
            piece = pltpu.roll(piece, a * wide, 1) if a else piece
            base = piece if base is None else base + piece
        for r in range(BAND):
            moved = pltpu.roll(base, r * wide, 1) if r else base
            tm_ref[layer, r * channels : (r + 1) * channels, :] = moved[:, :span].astype(BF16)

    span = t6_ref.shape[1]
    lanes = -(-span // 128) * 128
    base = None
    for a in range(3):
        few_ref[...] = jnp.zeros_like(few_ref)
        few_ref[:2, :wide] = last_ref[a].astype(F32)
        piece = jnp.concatenate([few_ref[...], jnp.zeros((8, lanes - 128), F32)], axis=1)
        piece = pltpu.roll(piece, a * wide, 1) if a else piece
        base = piece if base is None else base + piece
    for r in range(LAST_BAND):
        moved = pltpu.roll(base, r * wide, 1) if r else base
        for o in range(2):
            line_ref[o * LAST_BAND + r, :] = moved[o, :]
    t6_ref[...] = line_ref[:, :span].astype(BF16)

    span = t1_ref.shape[1]
    lanes = -(-span // 128) * 128
    taps = first_ref.shape[2]
    source = lax.broadcasted_iota(jnp.int32, (128, lanes), 0)
    target = lax.broadcasted_iota(jnp.int32, (128, lanes), 1)
    base = None
    for a in range(3):
        lane_ref[...] = jnp.zeros_like(lane_ref)
        lane_ref[:, :taps] = first_ref[a].astype(F32)
        pick = (target == source * rows_in + (EDGE - LAYERS + a)) & (source < taps)
        piece = jnp.dot(
            lane_ref[...].astype(BF16), pick.astype(F32).astype(BF16), preferred_element_type=F32
        )
        base = piece if base is None else base + piece
    for r in range(rows_out):
        moved = pltpu.roll(base, r, 1) if r else base
        t1_ref[r * channels : (r + 1) * channels, :] = moved[:, :span].astype(BF16)


def banded_weights(strip, first_weights, middle_weights, last_weights):
    count, _, channels, wide = middle_weights.shape
    rows_in = strip + 2 * EDGE
    rows_out = strip + 2 * (LAYERS - 1)
    return pl.pallas_call(
        functools.partial(band_kernel, strip),
        out_shape=(
            jax.ShapeDtypeStruct((rows_out * channels, first_weights.shape[2] * rows_in), BF16),
            jax.ShapeDtypeStruct((count, BAND * channels, (BAND + 2) * wide), BF16),
            jax.ShapeDtypeStruct((2 * LAST_BAND, (LAST_BAND + 2) * wide), BF16),
        ),
        in_specs=[VMEM] * 3,
        out_specs=(VMEM,) * 3,
        scratch_shapes=[
            pltpu.VMEM((channels, 128), F32),
            pltpu.VMEM((8, 128), F32),
            pltpu.VMEM((2 * LAST_BAND, -(-(LAST_BAND + 2) * wide // 128) * 128), F32),
        ],
        compiler_params=params(),
        cost_estimate=pl.CostEstimate(flops=10**9, bytes_accessed=3 * 10**6, transcendentals=0),
        name="bands",
    )(first_weights, middle_weights, last_weights)


def strip_kernel(
    where_ref, own_ref, top_ref, bottom_ref, t1_ref, tm_ref, t6_ref, out_ref, x_ref, b0_ref, ba_ref, bb_ref
):
    strip, width = own_ref.shape[1], own_ref.shape[2]
    channels = tm_ref.shape[1] // BAND
    rows_in = strip + 2 * EDGE
    is_first = where_ref[0] == 0
    is_last = where_ref[0] == where_ref[1] - 1
    lane = lax.broadcasted_iota(jnp.int32, (1, width), 1)

    def shifted(value):
        left = jnp.where(lane == 0, 0.0, pltpu.roll(value, 1, 1))
        right = jnp.where(lane == width - 1, 0.0, pltpu.roll(value, width - 1, 1))
        return left, value, right

    for part in range(2):
        x_ref[part, :EDGE, :] = jnp.where(is_first, 0.0, top_ref[part].astype(F32))
        x_ref[part, EDGE : EDGE + strip, :] = own_ref[part]
        x_ref[part, EDGE + strip :, :] = jnp.where(is_last, 0.0, bottom_ref[part].astype(F32))
    for part in range(2):
        for b, value in enumerate(shifted(x_ref[part].astype(BF16).astype(F32))):
            start = (b * 2 + part) * rows_in
            b0_ref[start : start + rows_in, :] = value.astype(BF16)

    def keep(result, row, margin, target):
        low = jnp.where(is_first, margin, 0)
        high = jnp.where(is_last, margin + strip, strip + 2 * margin)
        for j in range(BAND):
            value = jnp.maximum(result[j * channels : (j + 1) * channels, :], 0.0)
            inside = (row + j >= low) & (row + j < high)
            value = jnp.where(inside, value, 0.0)
            for b, moved in enumerate(shifted(value)):
                target[row + j, b * channels : (b + 1) * channels, :] = moved.astype(BF16)

    first_rows = strip + 2 * (LAYERS - 1)
    for start in range(0, first_rows, BAND):
        start = min(start, first_rows - BAND)
        result = jnp.dot(
            t1_ref[start * channels : (start + BAND) * channels, :], b0_ref[...], preferred_element_type=F32
        )
        keep(result, start, LAYERS - 1, ba_ref)

    source, target = ba_ref, bb_ref
    for depth in range(1, LAYERS - 1):
        margin = LAYERS - 1 - depth
        rows = strip + 2 * margin

        def group(number, carry, source=source, target=target, depth=depth, margin=margin, rows=rows):
            row = jnp.minimum(number * BAND, rows - BAND)
            taken = source[pl.ds(row, BAND + 2)]
            result = jnp.dot(
                tm_ref[depth - 1],
                taken.reshape(-1, width),
                preferred_element_type=F32,
            )
            keep(result, row, margin, target)
            return carry

        lax.fori_loop(0, -(-rows // BAND), group, 0)
        source, target = target, source

    for start in range(0, strip, LAST_BAND):
        taken = source[start : start + LAST_BAND + 2]
        result = jnp.dot(t6_ref[...], taken.reshape(-1, width), preferred_element_type=F32)
        for part in range(2):
            own = own_ref[part, start : start + LAST_BAND, :]
            noise = result[part * LAST_BAND : (part + 1) * LAST_BAND, :]
            out_ref[part, start : start + LAST_BAND, :] = own - 2.0 * noise


def prior_reflection(where, prior_state, top, bottom, bands):
    _, strip, width = prior_state.shape
    t1, tm, t6 = bands
    wide = tm.shape[2] // (BAND + 2)
    rows = strip + 2 * (LAYERS - 1)
    return pl.pallas_call(
        strip_kernel,
        out_shape=jax.ShapeDtypeStruct(prior_state.shape, F32),
        in_specs=[SMEM] + [VMEM] * 6,
        out_specs=VMEM,
        scratch_shapes=[
            pltpu.VMEM((2, strip + 2 * EDGE, width), F32),
            pltpu.VMEM((t1.shape[1], width), BF16),
            pltpu.VMEM((rows, wide, width), BF16),
            pltpu.VMEM((rows, wide, width), BF16),
        ],
        compiler_params=params(),
        cost_estimate=pl.CostEstimate(flops=8 * 10**9, bytes_accessed=3 * 10**6, transcendentals=0),
        name="denoise",
    )(where, prior_state, top, bottom, t1, tm, t6)


def gradient_kernel(
    corner_ref,
    flags_ref,
    middle_ref,
    left_ref,
    right_ref,
    measured_ref,
    probe_ref,
    forward_ref,
    backward_ref,
    up_ref,
    down_ref,
    own_ref,
    field_ref,
    total_ref,
    joined_ref,
    stacked_ref,
):
    count = measured_ref.shape[0]
    tall, wide = middle_ref.shape[1], middle_ref.shape[2] + 2 * HALO
    has_left = flags_ref[0] != 0
    has_right = flags_ref[1] != 0
    tile = middle_ref.shape[2]
    for part in range(2):
        field_ref[part, :tall, :HALO] = jnp.where(has_left, left_ref[part].astype(F32), 0.0)
        field_ref[part, :tall, HALO : HALO + tile] = middle_ref[part].astype(F32)
        field_ref[part, :tall, HALO + tile : wide] = jnp.where(has_right, right_ref[part].astype(F32), 0.0)
        field_ref[part, tall:, :] = jnp.zeros((8, wide + 128), F32)
        field_ref[part, :, wide:] = jnp.zeros((tall + 8, 128), F32)
    total_ref[...] = jnp.zeros_like(total_ref)

    lane = lax.broadcasted_iota(jnp.int32, (1, 128), 1)
    sub = lax.broadcasted_iota(jnp.int32, (1, 8, 1), 1)
    tall_load, wide_load = PROBE + 8, PROBE + 128

    def place_of(number):
        top, left = corner_ref[0, number], corner_ref[1, number]
        down, across = lax.rem(top, 8), lax.rem(left, 128)
        rows = pl.ds(pl.multiple_of(top - down, 8), tall_load)
        lanes = pl.ds(pl.multiple_of(left - across, 128), wide_load)
        return rows, lanes, down, across

    def window(part, number):
        rows, lanes, down, across = place_of(number)
        block = field_ref[part, rows, lanes]
        turned = [
            pltpu.roll(block[:, k : k + 128], lax.rem(128 - across, 128), 1) for k in range(0, wide_load, 128)
        ]
        block = jnp.concatenate(
            [jnp.where(lane < 128 - across, low, high) for low, high in zip(turned, turned[1:])], axis=1
        )
        block = pltpu.roll(block.reshape(tall_load // 8, 8, PROBE), lax.rem(8 - down, 8), 1)
        return jnp.where(sub < 8 - down, block[:-1], block[1:]).reshape(PROBE, PROBE)

    def add_window(part, number, terms):
        rows, lanes, down, across = place_of(number)
        block = pltpu.roll(terms.reshape(PROBE // 8, 8, PROBE), down, 1)
        empty = jnp.zeros((1, 8, PROBE), F32)
        block = jnp.where(
            sub >= down, jnp.concatenate([block, empty], axis=0), jnp.concatenate([empty, block], axis=0)
        ).reshape(tall_load, PROBE)
        turned = [pltpu.roll(block[:, k : k + 128], across, 1) for k in range(0, PROBE, 128)]
        empty = jnp.zeros((tall_load, 128), F32)
        block = jnp.concatenate(
            [jnp.where(lane >= across, high, low) for low, high in zip([empty, *turned], [*turned, empty])],
            axis=1,
        )
        total_ref[part, rows, lanes] = total_ref[part, rows, lanes] + block

    for number in range(count):
        real, imag = window(0, number), window(1, number)
        joined_ref[number, :, :PROBE] = (probe_ref[0] * real - probe_ref[1] * imag).astype(BF16)
        joined_ref[number, :, PROBE:] = (probe_ref[0] * imag + probe_ref[1] * real).astype(BF16)
    for number in range(count):
        half = jnp.dot(joined_ref[number], forward_ref[...], preferred_element_type=F32)
        stacked_ref[number, :PROBE, :] = half[:, :PROBE].astype(BF16)
        stacked_ref[number, PROBE:, :] = half[:, PROBE:].astype(BF16)
    for number in range(count):
        wave = jnp.dot(backward_ref[...], stacked_ref[number], preferred_element_type=F32)
        real, imag = wave[:PROBE], wave[PROBE:]
        power = jnp.maximum(real * real + imag * imag, MAGNITUDE_FLOOR * MAGNITUDE_FLOOR)
        retained = 1.0 - measured_ref[number] * lax.rsqrt(power)
        joined_ref[number, :, :PROBE] = (real * retained).astype(BF16)
        joined_ref[number, :, PROBE:] = (imag * retained).astype(BF16)
    for number in range(count):
        back = jnp.dot(joined_ref[number], backward_ref[...], preferred_element_type=F32)
        stacked_ref[number, :PROBE, :] = back[:, :PROBE].astype(BF16)
        stacked_ref[number, PROBE:, :] = back[:, PROBE:].astype(BF16)
    for number in range(count):
        field = jnp.dot(forward_ref[...], stacked_ref[number], preferred_element_type=F32)
        real, imag = field[:PROBE], field[PROBE:]
        add_window(0, number, probe_ref[0] * real + probe_ref[1] * imag)
        add_window(1, number, probe_ref[0] * imag - probe_ref[1] * real)
    for part in range(2):
        up_ref[part] = total_ref[part, :HALO, :wide].astype(BF16)
        own_ref[part] = total_ref[part, HALO : tall - HALO, :wide]
        down_ref[part] = total_ref[part, tall - HALO : tall, :wide].astype(BF16)


def gradient_terms(corners, flags, middle, left, right, measured, probe_field):
    tall = middle.shape[1]
    wide = middle.shape[2] + 2 * HALO
    count = measured.shape[0]
    forward, backward = dft_blocks()
    return pl.pallas_call(
        gradient_kernel,
        out_shape=(
            jax.ShapeDtypeStruct((2, HALO, wide), BF16),
            jax.ShapeDtypeStruct((2, HALO, wide), BF16),
            jax.ShapeDtypeStruct((2, tall - 2 * HALO, wide), F32),
        ),
        in_specs=[SMEM, SMEM] + [VMEM] * 7,
        out_specs=(VMEM,) * 3,
        scratch_shapes=[
            pltpu.VMEM((2, tall + 8, wide + 128), F32),
            pltpu.VMEM((2, tall + 8, wide + 128), F32),
            pltpu.VMEM((count, PROBE, 2 * PROBE), BF16),
            pltpu.VMEM((count, 2 * PROBE, PROBE), BF16),
        ],
        compiler_params=params(),
        cost_estimate=pl.CostEstimate(flops=5 * 10**9, bytes_accessed=4 * 10**6, transcendentals=0),
        name="gradient",
    )(corners, flags, middle, left, right, measured, probe_field, forward, backward)


def parcel_rows(strip, wide, tile, near):
    return 2 * strip * (wide // 128) + 2 * strip + (2 * tile if near else 0)


def gather_kernel(flags_ref, own_ref, above_ref, below_ref, data_ref, prior_ref, mine_ref, tile_ref, *parcels):
    columns = len(parcels) + 1
    strip = prior_ref.shape[1]
    wide = own_ref.shape[2]
    tile = data_ref.shape[2]
    above = flags_ref[0] != 0
    below = flags_ref[1] != 0
    column = flags_ref[2]
    for part in range(2):
        value = own_ref[part]
        value = value + jnp.where(above, above_ref[part].astype(F32), 0.0)
        value = value + jnp.where(below, below_ref[part].astype(F32), 0.0)
        tile_ref[part] = value

    def strip_terms(part, owner):
        start = pl.multiple_of(owner * strip, strip)
        terms = -2.0 * DATA_STEP * tile_ref[part, pl.ds(start, strip), :]
        data = data_ref[part, pl.ds(start, strip), :]
        return [
            terms[:, k * 128 : (k + 1) * 128] + data if k * 128 == HALO else terms[:, k * 128 : (k + 1) * 128]
            for k in range(wide // 128)
        ]

    for distance in range(columns):
        owner = lax.rem(column + distance, columns)
        row = 0
        for part in range(2):
            for k, terms in enumerate(strip_terms(part, owner)):
                if distance == 0:
                    mine_ref[part, :, k * 128 : (k + 1) * 128] = terms
                else:
                    parcels[distance - 1][row : row + strip, :] = terms.astype(BF16)
                row += strip
        if distance == 0:
            continue
        for part in range(2):
            lanes = pl.ds(pl.multiple_of(owner * tile, tile), tile)
            parcels[distance - 1][row : row + strip, :] = prior_ref[part, :, lanes].astype(BF16)
            row += strip
        for far, start in ((1, HALO + tile), (columns - 1, 0)):
            if distance == far:
                for part in range(2):
                    parcels[distance - 1][row : row + tile, :] = tile_ref[
                        part, :, start : start + HALO
                    ].astype(BF16)
                    row += tile


def gather_rows(flags, own, above, below, data_state, prior_reflect, columns):
    strip = prior_reflect.shape[1]
    _, tile, wide = own.shape
    shapes = [jax.ShapeDtypeStruct((2, strip, wide), F32), jax.ShapeDtypeStruct((2, tile, wide), F32)]
    for distance in range(1, columns):
        near = distance in (1, columns - 1)
        shapes.append(jax.ShapeDtypeStruct((parcel_rows(strip, wide, tile, near), 128), BF16))
    return pl.pallas_call(
        gather_kernel,
        out_shape=tuple(shapes),
        in_specs=[SMEM] + [VMEM] * 5,
        out_specs=(VMEM,) * len(shapes),
        compiler_params=params(),
        cost_estimate=pl.CostEstimate(flops=10**8, bytes_accessed=3 * 10**6, transcendentals=0),
        name="parcels",
    )(flags, own, above, below, data_state, prior_reflect)


def update_kernel(flags_ref, mine_ref, tile_ref, data_ref, state_ref, prior_ref, *rest):
    columns = len(rest) - 3 + 1
    parcels = rest[: columns - 1]
    data_out, prior_out, sum_ref = rest[columns - 1 :]
    strip = state_ref.shape[1]
    wide = mine_ref.shape[2]
    tile = data_ref.shape[2]
    column = flags_ref[2]
    blocks = wide // 128
    mixed = 1.0 - DATA_WEIGHT
    sum_ref[...] = jnp.zeros_like(sum_ref)
    for part in range(2):
        lanes = pl.ds(pl.multiple_of(column * tile, tile), wide)
        sum_ref[part, :, lanes] = mine_ref[part]
    for distance in range(1, columns):
        origin = lax.rem(column + columns - distance, columns)
        row = 0
        for part in range(2):
            for k in range(blocks):
                lanes = pl.ds(pl.multiple_of(origin * tile + k * 128, 128), 128)
                terms = parcels[distance - 1][row : row + strip, :].astype(F32)
                sum_ref[part, :, lanes] = sum_ref[part, :, lanes] + terms
                row += strip
    for part in range(2):
        reflect = sum_ref[part, :, HALO : HALO + state_ref.shape[2]]
        prior_out[part] = (
            (1.0 - RELAXATION) * state_ref[part]
            + (RELAXATION * 2.0 * DATA_WEIGHT) * reflect
            + (RELAXATION * (2.0 * mixed - 1.0)) * prior_ref[part]
        )
    near = 2 * strip * blocks + 2 * strip
    from_left = (column > 0, parcels[0])
    from_right = (column < columns - 1, parcels[columns - 2])
    for part in range(2):
        gradient = tile_ref[part, :, HALO : HALO + tile]
        for slot, (present, parcel) in enumerate((from_left, from_right)):
            start = near + part * tile
            if columns == 2:
                start = start + slot * 2 * tile
            terms = parcel[start : start + tile, :].astype(F32)
            gradient = gradient + jnp.where(present, terms, 0.0)
        data = data_ref[part]
        reflect = data - (2.0 * DATA_STEP) * gradient
        data_out[part] = (1.0 - RELAXATION) * data + (RELAXATION * (2.0 * DATA_WEIGHT - 1.0)) * reflect
    weight = RELAXATION * 2.0 * mixed
    for distance in range(columns):
        origin = lax.rem(column + columns - distance, columns)
        rows = pl.ds(pl.multiple_of(origin * strip, strip), strip)
        for part in range(2):
            if distance == 0:
                lanes = pl.ds(pl.multiple_of(column * tile, tile), tile)
                value = prior_ref[part, :, lanes]
            else:
                start = 2 * strip * blocks + part * strip
                value = parcels[distance - 1][start : start + strip, :].astype(F32)
            data_out[part, rows, :] = data_out[part, rows, :] + weight * value


def new_states(flags, mine, gradient, data_state, prior_state, prior_reflect, parcels):
    strip, width = prior_state.shape[1:]
    return pl.pallas_call(
        update_kernel,
        out_shape=(
            jax.ShapeDtypeStruct(data_state.shape, F32),
            jax.ShapeDtypeStruct(prior_state.shape, F32),
        ),
        in_specs=[SMEM] + [VMEM] * (5 + len(parcels)),
        out_specs=(VMEM,) * 2,
        scratch_shapes=[pltpu.VMEM((2, strip, width + 2 * HALO), F32)],
        compiler_params=params(),
        cost_estimate=pl.CostEstimate(flops=10**8, bytes_accessed=3 * 10**6, transcendentals=0),
        name="update",
    )(flags, mine, gradient, data_state, prior_state, prior_reflect, *parcels)


def on_device(
    probe_field,
    offsets,
    amplitudes,
    data_state,
    prior_state,
    first_weights,
    middle_weights,
    last_weights,
):
    tile_rows, tile_cols = data_state.shape[1:]
    strip = prior_state.shape[1]
    grid_rows, grid_cols = tile_rows // STEP, tile_cols // STEP
    columns = lax.axis_size("col")
    row, row_count = lax.axis_index(ROWS), lax.axis_size(ROWS)
    col = lax.axis_index("col")

    small = data_state.astype(BF16)
    from_above = ring(small, ROWS, 1)
    from_below = ring(small, ROWS, -1)
    top = ring(prior_state[:, strip - EDGE :].astype(BF16), STRIPS, 1)
    bottom = ring(prior_state[:, :EDGE].astype(BF16), STRIPS, -1)
    bands = banded_weights(strip, first_weights, middle_weights, last_weights)
    above, below = row > 0, row < row_count - 1
    zero = jnp.zeros_like(small)
    middle = jnp.concatenate(
        [jnp.where(above, from_above, zero), small, jnp.where(below, from_below, zero)], axis=1
    )
    left = ring(middle, "col", 1)
    right = ring(middle, "col", -1)

    base_rows = np.repeat(np.arange(grid_rows) * STEP + JITTER, grid_cols).astype(np.int32)
    base_cols = np.tile(np.arange(grid_cols) * STEP + JITTER, grid_rows).astype(np.int32)
    corners = offsets.reshape(2, -1) + np.stack([base_rows, base_cols])
    flags = jnp.stack([col > 0, col < columns - 1]).astype(jnp.int32)
    up, down, own = gradient_terms(
        corners, flags, middle, left, right, amplitudes.reshape(-1, PROBE, PROBE), probe_field
    )
    below_terms = ring(up, ROWS, -1)
    above_terms = ring(down, ROWS, 1)
    where = jnp.stack([row * columns + col, row_count * columns]).astype(jnp.int32)
    reflect = prior_reflection(where, prior_state, top, bottom, bands)
    flags = jnp.stack([above.astype(jnp.int32), below.astype(jnp.int32), col.astype(jnp.int32)])
    mine, gradient, *parcels = gather_rows(
        flags, own, above_terms, below_terms, data_state, reflect, columns
    )
    parcels = [ring(parcel, "col", number + 1) for number, parcel in enumerate(parcels)]
    return new_states(flags, mine, gradient, data_state, prior_state, reflect, parcels)


def solution(mesh):
    placed = (
        P(),
        P(None, ROWS, "col"),
        P(ROWS, "col", None, None),
        P(None, ROWS, "col"),
        P(None, STRIPS, None),
        P(),
        P(),
        P(),
    )
    return jax.shard_map(
        on_device,
        mesh=mesh,
        in_specs=placed,
        out_specs=(P(None, ROWS, "col"), P(None, STRIPS, None)),
        check_vma=False,
    )
```

```python
import functools
import math

import jax
import jax.numpy as jnp
import numpy as np
from jax import lax
from jax.experimental import pallas as pl
from jax.experimental.pallas import tpu as pltpu
from jax.sharding import PartitionSpec as P

PROBE = 256
STEP = 64
JITTER = 32
LAYERS = 6
HALO = 128
EDGE = 8
BAND = 3
LAST_BAND = 16

MAGNITUDE_FLOOR = 0.5
DATA_STEP = 0.125
DATA_WEIGHT = 0.6
RELAXATION = 0.5

ROWS = ("agent", "row")
STRIPS = ("agent", "row", "col")

VMEM = pl.BlockSpec(memory_space=pltpu.VMEM)
SMEM = pl.BlockSpec(memory_space=pltpu.SMEM)
BF16 = jnp.bfloat16
F32 = jnp.float32


def params(mib=48):
    return pltpu.CompilerParams(vmem_limit_bytes=mib * 1024 * 1024)


def dft_blocks():
    numbers = np.arange(PROBE)
    angles = (numbers[:, None] * numbers[None, :] % PROBE) * (2.0 * math.pi / PROBE)
    real = np.cos(angles) / math.sqrt(PROBE)
    imag = -np.sin(angles) / math.sqrt(PROBE)
    forward = np.block([[real, imag], [-imag, real]])
    return jnp.asarray(forward, BF16), jnp.asarray(forward.T.copy(), BF16)


def ring(value, axes, shift):
    count = lax.axis_size(axes)
    return lax.ppermute(value, axes, [(i, (i + shift) % count) for i in range(count)])


def swap(value, axes, start, closed):
    count = lax.axis_size(axes)
    pairs = []
    for i in range(count):
        other = ((i - start) ^ 1) + start
        pairs.append((i, other % count if closed else other if 0 <= other < count else i))
    return lax.ppermute(value, axes, pairs)


def cross(value, axes, distance):
    count = lax.axis_size(axes)
    return lax.ppermute(value, axes, [(i, i ^ distance) for i in range(count)])


def band_kernel(strip, first_ref, middle_ref, last_ref, t1_ref, tm_ref, t6_ref, lane_ref, few_ref, line_ref):
    channels = middle_ref.shape[2]
    wide = middle_ref.shape[3]
    rows_in = strip + 2 * EDGE
    rows_out = strip + 2 * (LAYERS - 1)
    lane_ref[...] = jnp.zeros_like(lane_ref)

    def widened(piece, lanes):
        height = piece.shape[0]
        lane_ref[:height, :wide] = piece
        value = lane_ref[:height, :]
        return jnp.concatenate([value, jnp.zeros((height, lanes - 128), F32)], axis=1)

    span = tm_ref.shape[2]
    lanes = -(-span // 128) * 128
    for layer in range(middle_ref.shape[0]):
        base = None
        for a in range(3):
            piece = widened(middle_ref[layer, a].astype(F32), lanes)
            piece = pltpu.roll(piece, a * wide, 1) if a else piece
            base = piece if base is None else base + piece
        for r in range(BAND):
            moved = pltpu.roll(base, r * wide, 1) if r else base
            tm_ref[layer, r * channels : (r + 1) * channels, :] = moved[:, :span].astype(BF16)

    span = t6_ref.shape[1]
    lanes = -(-span // 128) * 128
    base = None
    for a in range(3):
        few_ref[...] = jnp.zeros_like(few_ref)
        few_ref[:2, :wide] = last_ref[a].astype(F32)
        piece = jnp.concatenate([few_ref[...], jnp.zeros((8, lanes - 128), F32)], axis=1)
        piece = pltpu.roll(piece, a * wide, 1) if a else piece
        base = piece if base is None else base + piece
    for r in range(LAST_BAND):
        moved = pltpu.roll(base, r * wide, 1) if r else base
        for o in range(2):
            line_ref[o * LAST_BAND + r, :] = moved[o, :]
    t6_ref[...] = line_ref[:, :span].astype(BF16)

    span = t1_ref.shape[1]
    lanes = -(-span // 128) * 128
    taps = first_ref.shape[2]
    source = lax.broadcasted_iota(jnp.int32, (128, lanes), 0)
    target = lax.broadcasted_iota(jnp.int32, (128, lanes), 1)
    base = None
    for a in range(3):
        lane_ref[...] = jnp.zeros_like(lane_ref)
        lane_ref[:, :taps] = first_ref[a].astype(F32)
        pick = (target == source * rows_in + (EDGE - LAYERS + a)) & (source < taps)
        piece = jnp.dot(
            lane_ref[...].astype(BF16), pick.astype(F32).astype(BF16), preferred_element_type=F32
        )
        base = piece if base is None else base + piece
    for r in range(rows_out):
        moved = pltpu.roll(base, r, 1) if r else base
        t1_ref[r * channels : (r + 1) * channels, :] = moved[:, :span].astype(BF16)


def banded_weights(strip, first_weights, middle_weights, last_weights):
    count, _, channels, wide = middle_weights.shape
    rows_in = strip + 2 * EDGE
    rows_out = strip + 2 * (LAYERS - 1)
    return pl.pallas_call(
        functools.partial(band_kernel, strip),
        out_shape=(
            jax.ShapeDtypeStruct((rows_out * channels, first_weights.shape[2] * rows_in), BF16),
            jax.ShapeDtypeStruct((count, BAND * channels, (BAND + 2) * wide), BF16),
            jax.ShapeDtypeStruct((2 * LAST_BAND, (LAST_BAND + 2) * wide), BF16),
        ),
        in_specs=[VMEM] * 3,
        out_specs=(VMEM,) * 3,
        scratch_shapes=[
            pltpu.VMEM((channels, 128), F32),
            pltpu.VMEM((8, 128), F32),
            pltpu.VMEM((2 * LAST_BAND, -(-(LAST_BAND + 2) * wide // 128) * 128), F32),
        ],
        compiler_params=params(),
        cost_estimate=pl.CostEstimate(flops=10**9, bytes_accessed=3 * 10**6, transcendentals=0),
        name="bands",
    )(first_weights, middle_weights, last_weights)


def strip_kernel(
    where_ref, own_ref, top_ref, bottom_ref, t1_ref, tm_ref, t6_ref, out_ref, x_ref, b0_ref, ba_ref, bb_ref
):
    strip, width = own_ref.shape[1], own_ref.shape[2]
    channels = tm_ref.shape[1] // BAND
    rows_in = strip + 2 * EDGE
    is_first = where_ref[0] == 0
    is_last = where_ref[0] == where_ref[1] - 1
    lane = lax.broadcasted_iota(jnp.int32, (1, 128), 1)

    def shifted(value):
        tiles = [value[:, k : k + 128] for k in range(0, width, 128)]
        empty = jnp.zeros_like(tiles[0])
        down = [pltpu.roll(tile, 1, 1) for tile in tiles]
        up = [pltpu.roll(tile, 127, 1) for tile in tiles]
        left = [jnp.where(lane == 0, low, own) for low, own in zip([empty, *down], down)]
        right = [jnp.where(lane == 127, high, own) for high, own in zip([*up[1:], empty], up)]
        return jnp.concatenate(left, axis=1), value, jnp.concatenate(right, axis=1)

    for part in range(2):
        x_ref[part, :EDGE, :] = jnp.where(is_first, 0.0, top_ref[part].astype(F32))
        x_ref[part, EDGE : EDGE + strip, :] = own_ref[part]
        x_ref[part, EDGE + strip :, :] = jnp.where(is_last, 0.0, bottom_ref[part].astype(F32))
    for part in range(2):
        for b, value in enumerate(shifted(x_ref[part].astype(BF16).astype(F32))):
            start = (b * 2 + part) * rows_in
            b0_ref[start : start + rows_in, :] = value.astype(BF16)

    def keep(result, row, target):
        for j in range(BAND):
            value = jnp.maximum(result[j * channels : (j + 1) * channels, :], 0.0)
            for b, moved in enumerate(shifted(value)):
                target[row + j, b * channels : (b + 1) * channels, :] = moved.astype(BF16)

    def clear_outside(margin, target):
        @pl.when(is_first)
        def _():
            target[:margin] = jnp.zeros((margin, *target.shape[1:]), BF16)

        @pl.when(is_last)
        def _():
            target[margin + strip : strip + 2 * margin] = jnp.zeros((margin, *target.shape[1:]), BF16)

    margin = LAYERS - 1
    rows = strip + 2 * margin
    for start in range(0, rows, BAND):
        start = min(start, rows - BAND)
        result = jnp.dot(
            t1_ref[start * channels : (start + BAND) * channels, :], b0_ref[...], preferred_element_type=F32
        )
        keep(result, start, ba_ref)
    clear_outside(margin, ba_ref)

    source, target = ba_ref, bb_ref
    for depth in range(1, LAYERS - 1):
        margin = LAYERS - 1 - depth
        rows = strip + 2 * margin

        for start in range(0, rows, BAND):
            start = min(start, rows - BAND)
            taken = source[start : start + BAND + 2]
            result = jnp.dot(tm_ref[depth - 1], taken.reshape(-1, width), preferred_element_type=F32)
            keep(result, start, target)
        clear_outside(margin, target)
        source, target = target, source

    for start in range(0, strip, LAST_BAND):
        taken = source[start : start + LAST_BAND + 2]
        result = jnp.dot(t6_ref[...], taken.reshape(-1, width), preferred_element_type=F32)
        for part in range(2):
            own = own_ref[part, start : start + LAST_BAND, :]
            noise = result[part * LAST_BAND : (part + 1) * LAST_BAND, :]
            out_ref[part, start : start + LAST_BAND, :] = own - 2.0 * noise


def prior_reflection(where, prior_state, top, bottom, bands):
    _, strip, width = prior_state.shape
    t1, tm, t6 = bands
    wide = tm.shape[2] // (BAND + 2)
    rows = strip + 2 * (LAYERS - 1)
    return pl.pallas_call(
        strip_kernel,
        out_shape=jax.ShapeDtypeStruct(prior_state.shape, F32),
        in_specs=[SMEM] + [VMEM] * 6,
        out_specs=VMEM,
        scratch_shapes=[
            pltpu.VMEM((2, strip + 2 * EDGE, width), F32),
            pltpu.VMEM((t1.shape[1], width), BF16),
            pltpu.VMEM((rows, wide, width), BF16),
            pltpu.VMEM((rows, wide, width), BF16),
        ],
        compiler_params=params(),
        cost_estimate=pl.CostEstimate(flops=8 * 10**9, bytes_accessed=3 * 10**6, transcendentals=0),
        name="denoise",
    )(where, prior_state, top, bottom, t1, tm, t6)


def gradient_kernel(
    corner_ref,
    flags_ref,
    middle_ref,
    near_ref,
    far_ref,
    measured_ref,
    probe_ref,
    forward_ref,
    backward_ref,
    first_ref,
    second_ref,
    own_ref,
    field_ref,
    total_ref,
    joined_ref,
    stacked_ref,
):
    count = measured_ref.shape[0]
    tall, wide = middle_ref.shape[1], middle_ref.shape[2] + 2 * HALO
    odd_row, odd_column = lax.rem(flags_ref[0], 2), lax.rem(flags_ref[2], 2)
    alone = (flags_ref[2] == 0) | (flags_ref[2] == flags_ref[3] - 1)
    tile = middle_ref.shape[2]
    near_lanes = pl.ds(pl.multiple_of((1 - odd_column) * (HALO + tile), 128), HALO)
    far_lanes = pl.ds(pl.multiple_of(odd_column * (HALO + tile), 128), HALO)
    for part in range(2):
        field_ref[part, :tall, near_lanes] = near_ref[part].astype(F32)
        field_ref[part, :tall, HALO : HALO + tile] = middle_ref[part].astype(F32)
        field_ref[part, :tall, far_lanes] = jnp.where(alone, 0.0, far_ref[part].astype(F32))
        field_ref[part, tall:, :] = jnp.zeros((8, wide + 128), F32)
        field_ref[part, :, wide:] = jnp.zeros((tall + 8, 128), F32)
    total_ref[...] = jnp.zeros_like(total_ref)

    lane = lax.broadcasted_iota(jnp.int32, (1, 128), 1)
    sub = lax.broadcasted_iota(jnp.int32, (1, 8, 1), 1)
    tall_load, wide_load = PROBE + 8, PROBE + 128

    def place_of(number):
        top, left = corner_ref[0, number], corner_ref[1, number]
        down, across = lax.rem(top, 8), lax.rem(left, 128)
        rows = pl.ds(pl.multiple_of(top - down, 8), tall_load)
        lanes = pl.ds(pl.multiple_of(left - across, 128), wide_load)
        return rows, lanes, down, across

    def window(part, number):
        rows, lanes, down, across = place_of(number)
        block = field_ref[part, rows, lanes]
        turned = [
            pltpu.roll(block[:, k : k + 128], lax.rem(128 - across, 128), 1) for k in range(0, wide_load, 128)
        ]
        block = jnp.concatenate(
            [jnp.where(lane < 128 - across, low, high) for low, high in zip(turned, turned[1:])], axis=1
        )
        block = pltpu.roll(block.reshape(tall_load // 8, 8, PROBE), lax.rem(8 - down, 8), 1)
        return jnp.where(sub < 8 - down, block[:-1], block[1:]).reshape(PROBE, PROBE)

    def add_window(part, number, terms):
        rows, lanes, down, across = place_of(number)
        block = pltpu.roll(terms.reshape(PROBE // 8, 8, PROBE), down, 1)
        empty = jnp.zeros((1, 8, PROBE), F32)
        block = jnp.where(
            sub >= down, jnp.concatenate([block, empty], axis=0), jnp.concatenate([empty, block], axis=0)
        ).reshape(tall_load, PROBE)
        turned = [pltpu.roll(block[:, k : k + 128], across, 1) for k in range(0, PROBE, 128)]
        empty = jnp.zeros((tall_load, 128), F32)
        block = jnp.concatenate(
            [jnp.where(lane >= across, high, low) for low, high in zip([empty, *turned], [*turned, empty])],
            axis=1,
        )
        total_ref[part, rows, lanes] = total_ref[part, rows, lanes] + block

    for number in range(count):
        real, imag = window(0, number), window(1, number)
        joined_ref[number, :, :PROBE] = (probe_ref[0] * real - probe_ref[1] * imag).astype(BF16)
        joined_ref[number, :, PROBE:] = (probe_ref[0] * imag + probe_ref[1] * real).astype(BF16)
    for number in range(count):
        half = jnp.dot(joined_ref[number], forward_ref[...], preferred_element_type=F32)
        stacked_ref[number, :PROBE, :] = half[:, :PROBE].astype(BF16)
        stacked_ref[number, PROBE:, :] = half[:, PROBE:].astype(BF16)
    for number in range(count):
        wave = jnp.dot(backward_ref[...], stacked_ref[number], preferred_element_type=F32)
        real, imag = wave[:PROBE], wave[PROBE:]
        power = jnp.maximum(real * real + imag * imag, MAGNITUDE_FLOOR * MAGNITUDE_FLOOR)
        retained = 1.0 - measured_ref[number] * lax.rsqrt(power)
        joined_ref[number, :, :PROBE] = (real * retained).astype(BF16)
        joined_ref[number, :, PROBE:] = (imag * retained).astype(BF16)
    for number in range(count):
        back = jnp.dot(joined_ref[number], backward_ref[...], preferred_element_type=F32)
        stacked_ref[number, :PROBE, :] = back[:, :PROBE].astype(BF16)
        stacked_ref[number, PROBE:, :] = back[:, PROBE:].astype(BF16)
    for number in range(count):
        field = jnp.dot(forward_ref[...], stacked_ref[number], preferred_element_type=F32)
        real, imag = field[:PROBE], field[PROBE:]
        add_window(0, number, probe_ref[0] * real + probe_ref[1] * imag)
        add_window(1, number, probe_ref[0] * imag - probe_ref[1] * real)
    first_rows = pl.ds(pl.multiple_of((1 - odd_row) * (tall - HALO), 8), HALO)
    second_rows = pl.ds(pl.multiple_of(odd_row * (tall - HALO), 8), HALO)
    for part in range(2):
        first_ref[part] = total_ref[part, first_rows, :wide].astype(BF16)
        second_ref[part] = total_ref[part, second_rows, :wide].astype(BF16)
        own_ref[part] = total_ref[part, HALO : tall - HALO, :wide]


def gradient_terms(corners, flags, middle, near, far, measured, probe_field):
    tall = middle.shape[1]
    wide = middle.shape[2] + 2 * HALO
    count = measured.shape[0]
    forward, backward = dft_blocks()
    return pl.pallas_call(
        gradient_kernel,
        out_shape=(
            jax.ShapeDtypeStruct((2, HALO, wide), BF16),
            jax.ShapeDtypeStruct((2, HALO, wide), BF16),
            jax.ShapeDtypeStruct((2, tall - 2 * HALO, wide), F32),
        ),
        in_specs=[SMEM, SMEM] + [VMEM] * 7,
        out_specs=(VMEM,) * 3,
        scratch_shapes=[
            pltpu.VMEM((2, tall + 8, wide + 128), F32),
            pltpu.VMEM((2, tall + 8, wide + 128), F32),
            pltpu.VMEM((count, PROBE, 2 * PROBE), BF16),
            pltpu.VMEM((count, 2 * PROBE, PROBE), BF16),
        ],
        compiler_params=params(),
        cost_estimate=pl.CostEstimate(flops=5 * 10**9, bytes_accessed=4 * 10**6, transcendentals=0),
        name="gradient",
    )(corners, flags, middle, near, far, measured, probe_field, forward, backward)


DATA_GRADIENT = -2.0 * DATA_STEP * RELAXATION * (2.0 * DATA_WEIGHT - 1.0)
DATA_PRIOR = 2.0 * RELAXATION * (1.0 - DATA_WEIGHT)
PRIOR_DATA = 2.0 * RELAXATION * DATA_WEIGHT
PRIOR_PRIOR = RELAXATION * (1.0 - 2.0 * DATA_WEIGHT)


def can_touch(distance):
    return distance & (distance + 1) == 0


def parcel_rows(strip, wide, tile, distance):
    return 2 * strip * (wide // 128) + 2 * strip + (2 * tile if can_touch(distance) else 0)


def strip_terms(tile_ref, data_ref, part, owner, strip):
    start = pl.multiple_of(owner * strip, strip)
    terms = (PRIOR_DATA * -2.0 * DATA_STEP) * tile_ref[part, pl.ds(start, strip), :]
    data = PRIOR_DATA * data_ref[part, pl.ds(start, strip), :]
    pieces = [terms[:, k : k + 128] for k in range(0, terms.shape[1], 128)]
    pieces[HALO // 128] = pieces[HALO // 128] + data
    return pieces


def parcel_kernel(flags_ref, own_ref, first_ref, second_ref, data_ref, prior_ref, tile_ref, *parcels):
    strip = prior_ref.shape[1]
    tile = data_ref.shape[2]
    end = (flags_ref[0] == 0) | (flags_ref[0] == flags_ref[1] - 1)
    column = flags_ref[2]
    for part in range(2):
        value = own_ref[part] + first_ref[part].astype(F32)
        tile_ref[part] = value + jnp.where(end, 0.0, second_ref[part].astype(F32))
    for distance, parcel in enumerate(parcels, 1):
        owner = column ^ distance
        row = 0
        for part in range(2):
            for terms in strip_terms(tile_ref, data_ref, part, owner, strip):
                parcel[row : row + strip, :] = terms.astype(BF16)
                row += strip
        for part in range(2):
            lanes = pl.ds(pl.multiple_of(owner * tile, tile), tile)
            parcel[row : row + strip, :] = (DATA_PRIOR * prior_ref[part, :, lanes]).astype(BF16)
            row += strip
        if can_touch(distance):
            lanes = pl.ds(pl.multiple_of(jnp.where(owner > column, HALO + tile, 0), 128), HALO)
            for part in range(2):
                parcel[row : row + tile, :] = (DATA_GRADIENT * tile_ref[part, :, lanes]).astype(BF16)
                row += tile


def parcels_of(flags, own, first, second, data_state, prior_reflect, columns):
    strip = prior_reflect.shape[1]
    _, tile, wide = own.shape
    shapes = [jax.ShapeDtypeStruct((2, tile, wide), F32)]
    for distance in range(1, columns):
        shapes.append(jax.ShapeDtypeStruct((parcel_rows(strip, wide, tile, distance), 128), BF16))
    return pl.pallas_call(
        parcel_kernel,
        out_shape=tuple(shapes),
        in_specs=[SMEM] + [VMEM] * 5,
        out_specs=(VMEM,) * len(shapes),
        compiler_params=params(),
        cost_estimate=pl.CostEstimate(flops=10**8, bytes_accessed=3 * 10**6, transcendentals=0),
        name="parcels",
    )(flags, own, first, second, data_state, prior_reflect)


def base_kernel(flags_ref, tile_ref, data_ref, state_ref, prior_ref, data_out, prior_out):
    strip = state_ref.shape[1]
    tile = data_ref.shape[2]
    column = flags_ref[2]
    own_rows = pl.ds(pl.multiple_of(column * strip, strip), strip)
    own_lanes = pl.ds(pl.multiple_of(column * tile, tile), tile)
    for part in range(2):
        data_out[part] = (
            (1.0 - RELAXATION) + RELAXATION * (2.0 * DATA_WEIGHT - 1.0)
        ) * data_ref[part] + DATA_GRADIENT * tile_ref[part, :, HALO : HALO + tile]
        data_out[part, own_rows, :] = data_out[part, own_rows, :] + DATA_PRIOR * prior_ref[part, :, own_lanes]
        width = state_ref.shape[2]
        inner = slice(HALO, HALO + width)
        prior_out[part, :, :HALO] = jnp.zeros((strip, HALO), F32)
        prior_out[part, :, HALO + width :] = jnp.zeros((strip, HALO), F32)
        prior_out[part, :, inner] = (1.0 - RELAXATION) * state_ref[part] + PRIOR_PRIOR * prior_ref[part]
        for k, terms in enumerate(strip_terms(tile_ref, data_ref, part, column, strip)):
            lanes = pl.ds(pl.multiple_of(column * tile + k * 128, 128), 128)
            prior_out[part, :, lanes] = prior_out[part, :, lanes] + terms


def own_terms(flags, gradient, data_state, prior_state, prior_reflect):
    _, strip, width = prior_state.shape
    return pl.pallas_call(
        base_kernel,
        out_shape=(
            jax.ShapeDtypeStruct(data_state.shape, F32),
            jax.ShapeDtypeStruct((2, strip, width + 2 * HALO), F32),
        ),
        in_specs=[SMEM] + [VMEM] * 4,
        out_specs=(VMEM,) * 2,
        compiler_params=params(),
        cost_estimate=pl.CostEstimate(flops=10**9, bytes_accessed=3 * 10**6, transcendentals=0),
        name="base",
    )(flags, gradient, data_state, prior_state, prior_reflect)


def update_kernel(flags_ref, data_base, prior_base, *rest):
    *parcels, data_out, prior_out, data_ref, prior_ref, padded_ref, sems = rest
    strip, width = prior_ref.shape[1], prior_ref.shape[2]
    tile = data_ref.shape[2]
    column = flags_ref[2]
    blocks = 2 * HALO // 128 + tile // 128
    data_ref[...] = data_base[...]
    padded_ref[...] = prior_base[...]
    for distance, parcel in enumerate(parcels, 1):
        origin = column ^ distance
        row = 0
        for part in range(2):
            for k in range(blocks):
                lanes = pl.ds(pl.multiple_of(origin * tile + k * 128, 128), 128)
                terms = parcel[row : row + strip, :].astype(F32)
                padded_ref[part, :, lanes] = padded_ref[part, :, lanes] + terms
                row += strip
    prior_ref[...] = padded_ref[:, :, HALO : HALO + width]
    copy_prior = pltpu.make_async_copy(prior_ref, prior_out, sems.at[0])
    copy_prior.start()
    for distance, parcel in enumerate(parcels, 1):
        origin = column ^ distance
        row = 2 * strip * blocks
        rows = pl.ds(pl.multiple_of(origin * strip, strip), strip)
        for part in range(2):
            data_ref[part, rows, :] = data_ref[part, rows, :] + parcel[row : row + strip, :].astype(F32)
            row += strip
        if can_touch(distance):
            touching = (origin == column + 1) | (origin == column - 1)
            for part in range(2):
                terms = parcel[row : row + tile, :].astype(F32)
                data_ref[part] = data_ref[part] + jnp.where(touching, terms, 0.0)
                row += tile
    copy_data = pltpu.make_async_copy(data_ref, data_out, sems.at[1])
    copy_data.start()
    copy_prior.wait()
    copy_data.wait()


def new_states(flags, data_base, prior_base, parcels):
    _, strip, padded = prior_base.shape
    width = padded - 2 * HALO
    return pl.pallas_call(
        update_kernel,
        out_shape=(
            jax.ShapeDtypeStruct(data_base.shape, F32),
            jax.ShapeDtypeStruct((2, strip, width), F32),
        ),
        in_specs=[SMEM] + [VMEM] * (2 + len(parcels)),
        out_specs=(pl.BlockSpec(memory_space=pl.ANY),) * 2,
        scratch_shapes=[
            pltpu.VMEM(data_base.shape, F32),
            pltpu.VMEM((2, strip, width), F32),
            pltpu.VMEM(prior_base.shape, F32),
            pltpu.SemaphoreType.DMA((2,)),
        ],
        compiler_params=params(),
        cost_estimate=pl.CostEstimate(flops=10**8, bytes_accessed=3 * 10**6, transcendentals=0),
        name="update",
    )(flags, data_base, prior_base, *parcels)


def on_device(
    probe_field,
    offsets,
    amplitudes,
    data_state,
    prior_state,
    first_weights,
    middle_weights,
    last_weights,
):
    tile_rows, tile_cols = data_state.shape[1:]
    strip = prior_state.shape[1]
    grid_rows, grid_cols = tile_rows // STEP, tile_cols // STEP
    row, row_count = lax.axis_index(ROWS), lax.axis_size(ROWS)
    col, columns = lax.axis_index("col"), lax.axis_size("col")

    small = data_state.astype(BF16)
    first = swap(small, ROWS, 0, True)
    second = swap(small, ROWS, 1, True)
    bands = banded_weights(strip, first_weights, middle_weights, last_weights)
    zero = jnp.zeros_like(small)
    second = jnp.where((row == 0) | (row == row_count - 1), zero, second)
    odd = row % 2 == 1
    middle = jnp.concatenate([jnp.where(odd, first, second), small, jnp.where(odd, second, first)], axis=1)
    near = swap(middle, "col", 0, False)
    far = swap(middle, "col", 1, False)
    low, high, _ = lax.optimization_barrier((prior_state[:, strip - EDGE :], prior_state[:, :EDGE], middle))
    top = ring(low.astype(BF16), STRIPS, 1)
    bottom = ring(high.astype(BF16), STRIPS, -1)

    base_rows = np.repeat(np.arange(grid_rows) * STEP + JITTER, grid_cols).astype(np.int32)
    base_cols = np.tile(np.arange(grid_cols) * STEP + JITTER, grid_rows).astype(np.int32)
    corners = offsets.reshape(2, -1) + np.stack([base_rows, base_cols])
    flags = jnp.stack([row, jnp.int32(row_count), col, jnp.int32(columns)]).astype(jnp.int32)
    first, second, own = gradient_terms(
        corners, flags, middle, near, far, amplitudes.reshape(-1, PROBE, PROBE), probe_field
    )
    first = swap(first, ROWS, 0, True)
    second = swap(second, ROWS, 1, True)
    where = jnp.stack([row * columns + col, jnp.int32(row_count * columns)]).astype(jnp.int32)
    reflect = prior_reflection(where, prior_state, top, bottom, bands)
    gradient, *parcels = parcels_of(flags, own, first, second, data_state, reflect, columns)
    bases = own_terms(flags, gradient, data_state, prior_state, reflect)
    parcels = [cross(parcel, "col", distance) for distance, parcel in enumerate(parcels, 1)]
    return new_states(flags, *bases, parcels)


def solution(mesh):
    placed = (
        P(),
        P(None, ROWS, "col"),
        P(ROWS, "col", None, None),
        P(None, ROWS, "col"),
        P(None, STRIPS, None),
        P(),
        P(),
        P(),
    )
    return jax.shard_map(
        on_device,
        mesh=mesh,
        in_specs=placed,
        out_specs=(P(None, ROWS, "col"), P(None, STRIPS, None)),
        check_vma=False,
    )
```

```python
import functools
import math

import jax
import jax.numpy as jnp
import numpy as np
from jax import lax
from jax.experimental import pallas as pl
from jax.experimental.pallas import tpu as pltpu
from jax.sharding import PartitionSpec as P

PROBE = 256
STEP = 64
JITTER = 32
LAYERS = 6
HALO = 128
EDGE = 8
BAND = 3
LAST_BAND = 16
CHUNK = 32

MAGNITUDE_FLOOR = 0.5
DATA_STEP = 0.125
DATA_WEIGHT = 0.6
RELAXATION = 0.5

ROWS = ("agent", "row")
STRIPS = ("agent", "row", "col")

VMEM = pl.BlockSpec(memory_space=pltpu.VMEM)
SMEM = pl.BlockSpec(memory_space=pltpu.SMEM)
BF16 = jnp.bfloat16
F32 = jnp.float32


def params(mib=48):
    return pltpu.CompilerParams(vmem_limit_bytes=mib * 1024 * 1024)


def dft_blocks():
    numbers = np.arange(PROBE)
    angles = (numbers[:, None] * numbers[None, :] % PROBE) * (2.0 * math.pi / PROBE)
    real = np.cos(angles) / math.sqrt(PROBE)
    imag = -np.sin(angles) / math.sqrt(PROBE)
    forward = np.block([[real, imag], [-imag, real]])
    return jnp.asarray(forward, BF16), jnp.asarray(forward.T.copy(), BF16)


def swap(value, axes, start, closed):
    count = lax.axis_size(axes)
    pairs = []
    for i in range(count):
        other = ((i - start) ^ 1) + start
        pairs.append((i, other % count if closed else other if 0 <= other < count else i))
    return lax.ppermute(value, axes, pairs)


def cross(value, axes, distance):
    count = lax.axis_size(axes)
    return lax.ppermute(value, axes, [(i, i ^ distance) for i in range(count)])


def tile_place():
    return lax.axis_index(ROWS), lax.axis_size(ROWS), lax.axis_index("col"), lax.axis_size("col")


def edge_rows(prior_state):
    return EDGE * prior_state.shape[2] // 128


def put_edge(target, part, start, edge):
    for k in range(0, edge.shape[1], 128):
        target[part, start : start + EDGE, :] = edge[:, k : k + 128].astype(BF16)
        start += EDGE


def packed(data_state, prior_state):
    _, _, column, columns = tile_place()
    strip, width = prior_state.shape[1:]
    low, high = prior_state[:, :EDGE], prior_state[:, strip - EDGE :]
    edge = jnp.where(column == columns - 1, high, low)
    pieces = [edge[:, :, k : k + 128] for k in range(0, width, 128)]
    return jnp.concatenate([data_state, *pieces], axis=1).astype(BF16)


def widen_kernel(own_ref, first_ref, second_ref, prior_ref, near_ref, far_ref, edge_ref):
    tile, strip = own_ref.shape[2], prior_ref.shape[1]
    row, row_count, column, columns = tile_place()
    odd_row, odd_column = lax.rem(row, 2), lax.rem(column, 2)
    end = (row == 0) | (row == row_count - 1)
    first_rows = pl.ds(pl.multiple_of((1 - odd_row) * 2 * tile, tile), tile)
    second_rows = pl.ds(pl.multiple_of(odd_row * 2 * tile, tile), tile)
    for part in range(2):
        second = jnp.where(end, 0.0, second_ref[part, :tile, :].astype(F32)).astype(BF16)
        for target in (near_ref, far_ref):
            target[part, first_rows, :] = first_ref[part, :tile, :]
            target[part, tile : 2 * tile, :] = own_ref[part, :tile, :]
            target[part, second_rows, :] = second
        low, high = prior_ref[part, :EDGE, :], prior_ref[part, strip - EDGE :, :]
        put_edge(near_ref, part, 3 * tile, jnp.where(odd_column == 1, low, high))
        put_edge(edge_ref, part, 0, jnp.where(odd_column == 1, high, low))
        one, two = first_ref[part, tile:, :].astype(F32), second_ref[part, tile:, :].astype(F32)
        above, below = jnp.where(odd_row == 1, one, two), jnp.where(odd_row == 1, two, one)
        mine = edge_ref[part].astype(F32)
        mine = jnp.where(column == columns - 1, above, jnp.where(column == 0, below, mine))
        edge_ref[part] = mine.astype(BF16)


def widened(own, first, second, prior_state):
    tile, edge = own.shape[2], edge_rows(prior_state)
    return pl.pallas_call(
        widen_kernel,
        out_shape=(
            jax.ShapeDtypeStruct((2, 3 * tile + edge, tile), BF16),
            jax.ShapeDtypeStruct((2, 3 * tile, tile), BF16),
            jax.ShapeDtypeStruct((2, edge, tile), BF16),
        ),
        in_specs=[VMEM] * 4,
        out_specs=(VMEM,) * 3,
        compiler_params=params(),
        cost_estimate=pl.CostEstimate(flops=10**6, bytes_accessed=10**6, transcendentals=0),
        name="widen",
    )(own, first, second, prior_state)


def band_kernel(strip, first_ref, middle_ref, last_ref, t1_ref, tm_ref, t6_ref, lane_ref, few_ref, line_ref):
    channels = middle_ref.shape[2]
    wide = middle_ref.shape[3]
    rows_in = strip + 2 * EDGE
    rows_out = strip + 2 * (LAYERS - 1)
    lane_ref[...] = jnp.zeros_like(lane_ref)

    def widened(piece, lanes):
        height = piece.shape[0]
        lane_ref[:height, :wide] = piece
        value = lane_ref[:height, :]
        return jnp.concatenate([value, jnp.zeros((height, lanes - 128), F32)], axis=1)

    span = tm_ref.shape[2]
    lanes = -(-span // 128) * 128
    for layer in range(middle_ref.shape[0]):
        base = None
        for a in range(3):
            piece = widened(middle_ref[layer, a].astype(F32), lanes)
            piece = pltpu.roll(piece, a * wide, 1) if a else piece
            base = piece if base is None else base + piece
        for r in range(BAND):
            moved = pltpu.roll(base, r * wide, 1) if r else base
            tm_ref[layer, r * channels : (r + 1) * channels, :] = moved[:, :span].astype(BF16)

    span = t6_ref.shape[1]
    lanes = -(-span // 128) * 128
    base = None
    for a in range(3):
        few_ref[...] = jnp.zeros_like(few_ref)
        few_ref[:2, :wide] = last_ref[a].astype(F32)
        piece = jnp.concatenate([few_ref[...], jnp.zeros((8, lanes - 128), F32)], axis=1)
        piece = pltpu.roll(piece, a * wide, 1) if a else piece
        base = piece if base is None else base + piece
    for r in range(LAST_BAND):
        moved = pltpu.roll(base, r * wide, 1) if r else base
        for o in range(2):
            line_ref[o * LAST_BAND + r, :] = moved[o, :]
    t6_ref[...] = line_ref[:, :span].astype(BF16)

    span = t1_ref.shape[1]
    lanes = -(-span // 128) * 128
    taps = first_ref.shape[2]
    source = lax.broadcasted_iota(jnp.int32, (128, lanes), 0)
    target = lax.broadcasted_iota(jnp.int32, (128, lanes), 1)
    base = None
    for a in range(3):
        lane_ref[...] = jnp.zeros_like(lane_ref)
        lane_ref[:, :taps] = first_ref[a].astype(F32)
        pick = (target == source * rows_in + (EDGE - LAYERS + a)) & (source < taps)
        piece = jnp.dot(
            lane_ref[...].astype(BF16), pick.astype(F32).astype(BF16), preferred_element_type=F32
        )
        base = piece if base is None else base + piece
    for r in range(rows_out):
        moved = pltpu.roll(base, r, 1) if r else base
        t1_ref[r * channels : (r + 1) * channels, :] = moved[:, :span].astype(BF16)


def banded_weights(strip, first_weights, middle_weights, last_weights):
    count, _, channels, wide = middle_weights.shape
    rows_in = strip + 2 * EDGE
    rows_out = strip + 2 * (LAYERS - 1)
    return pl.pallas_call(
        functools.partial(band_kernel, strip),
        out_shape=(
            jax.ShapeDtypeStruct((rows_out * channels, first_weights.shape[2] * rows_in), BF16),
            jax.ShapeDtypeStruct((count, BAND * channels, (BAND + 2) * wide), BF16),
            jax.ShapeDtypeStruct((2 * LAST_BAND, (LAST_BAND + 2) * wide), BF16),
        ),
        in_specs=[VMEM] * 3,
        out_specs=(VMEM,) * 3,
        scratch_shapes=[
            pltpu.VMEM((channels, 128), F32),
            pltpu.VMEM((8, 128), F32),
            pltpu.VMEM((2 * LAST_BAND, -(-(LAST_BAND + 2) * wide // 128) * 128), F32),
        ],
        compiler_params=params(),
        cost_estimate=pl.CostEstimate(flops=10**9, bytes_accessed=3 * 10**6, transcendentals=0),
        name="bands",
    )(first_weights, middle_weights, last_weights)


def strip_kernel(
    own_ref, near_ref, edge_ref, t1_ref, tm_ref, t6_ref, out_ref, x_ref, b0_ref, ba_ref, bb_ref
):
    strip, width = own_ref.shape[1], own_ref.shape[2]
    channels = tm_ref.shape[1] // BAND
    rows_in = strip + 2 * EDGE
    row, row_count, column, columns = tile_place()
    number = row * columns + column
    is_first = number == 0
    is_last = number == row_count * columns - 1
    odd = lax.rem(column, 2) == 1
    lane = lax.broadcasted_iota(jnp.int32, (1, 128), 1)

    def shifted(value):
        tiles = [value[:, k : k + 128] for k in range(0, width, 128)]
        empty = jnp.zeros_like(tiles[0])
        down = [pltpu.roll(tile, 1, 1) for tile in tiles]
        up = [pltpu.roll(tile, 127, 1) for tile in tiles]
        left = [jnp.where(lane == 0, low, own) for low, own in zip([empty, *down], down)]
        right = [jnp.where(lane == 127, high, own) for high, own in zip([*up[1:], empty], up)]
        return jnp.concatenate(left, axis=1), value, jnp.concatenate(right, axis=1)

    for part in range(2):
        for k in range(width // 128):
            start = near_ref.shape[1] - edge_ref.shape[1] + k * EDGE
            near = near_ref[part, start : start + EDGE, :].astype(F32)
            far = edge_ref[part, k * EDGE : (k + 1) * EDGE, :].astype(F32)
            lanes = slice(k * 128, (k + 1) * 128)
            x_ref[part, :EDGE, lanes] = jnp.where(is_first, 0.0, jnp.where(odd, near, far))
            x_ref[part, EDGE + strip :, lanes] = jnp.where(is_last, 0.0, jnp.where(odd, far, near))
        x_ref[part, EDGE : EDGE + strip, :] = own_ref[part]
    for part in range(2):
        for b, value in enumerate(shifted(x_ref[part].astype(BF16).astype(F32))):
            start = (b * 2 + part) * rows_in
            b0_ref[start : start + rows_in, :] = value.astype(BF16)

    def keep(result, row, target):
        for j in range(BAND):
            value = jnp.maximum(result[j * channels : (j + 1) * channels, :], 0.0)
            for b, moved in enumerate(shifted(value)):
                target[row + j, b * channels : (b + 1) * channels, :] = moved.astype(BF16)

    def clear_outside(margin, target):
        @pl.when(is_first)
        def _():
            target[:margin] = jnp.zeros((margin, *target.shape[1:]), BF16)

        @pl.when(is_last)
        def _():
            target[margin + strip : strip + 2 * margin] = jnp.zeros((margin, *target.shape[1:]), BF16)

    margin = LAYERS - 1
    rows = strip + 2 * margin
    for start in range(0, rows, BAND):
        start = min(start, rows - BAND)
        result = jnp.dot(
            t1_ref[start * channels : (start + BAND) * channels, :], b0_ref[...], preferred_element_type=F32
        )
        keep(result, start, ba_ref)
    clear_outside(margin, ba_ref)

    source, target = ba_ref, bb_ref
    for depth in range(1, LAYERS - 1):
        margin = LAYERS - 1 - depth
        rows = strip + 2 * margin

        for start in range(0, rows, BAND):
            start = min(start, rows - BAND)
            taken = source[start : start + BAND + 2]
            result = jnp.dot(tm_ref[depth - 1], taken.reshape(-1, width), preferred_element_type=F32)
            keep(result, start, target)
        clear_outside(margin, target)
        source, target = target, source

    for start in range(0, strip, LAST_BAND):
        taken = source[start : start + LAST_BAND + 2]
        result = jnp.dot(t6_ref[...], taken.reshape(-1, width), preferred_element_type=F32)
        for part in range(2):
            own = own_ref[part, start : start + LAST_BAND, :]
            noise = result[part * LAST_BAND : (part + 1) * LAST_BAND, :]
            out_ref[part, start : start + LAST_BAND, :] = own - 2.0 * noise


def prior_reflection(prior_state, near, edge, bands):
    _, strip, width = prior_state.shape
    t1, tm, t6 = bands
    wide = tm.shape[2] // (BAND + 2)
    rows = strip + 2 * (LAYERS - 1)
    return pl.pallas_call(
        strip_kernel,
        out_shape=jax.ShapeDtypeStruct(prior_state.shape, F32),
        in_specs=[VMEM] * 6,
        out_specs=VMEM,
        scratch_shapes=[
            pltpu.VMEM((2, strip + 2 * EDGE, width), F32),
            pltpu.VMEM((t1.shape[1], width), BF16),
            pltpu.VMEM((rows, wide, width), BF16),
            pltpu.VMEM((rows, wide, width), BF16),
        ],
        compiler_params=params(),
        cost_estimate=pl.CostEstimate(flops=8 * 10**9, bytes_accessed=3 * 10**6, transcendentals=0),
        name="denoise",
    )(prior_state, near, edge, t1, tm, t6)


def gradient_kernel(
    offset_ref,
    middle_ref,
    near_ref,
    far_ref,
    measured_ref,
    probe_ref,
    forward_ref,
    backward_ref,
    first_ref,
    second_ref,
    own_ref,
    field_ref,
    total_ref,
    joined_ref,
    stacked_ref,
):
    count = measured_ref.shape[0]
    tall, wide = middle_ref.shape[1], middle_ref.shape[2] + 2 * HALO
    row, _, column, columns = tile_place()
    odd_row, odd_column = lax.rem(row, 2), lax.rem(column, 2)
    alone = (column == 0) | (column == columns - 1)
    tile = middle_ref.shape[2]
    near_lanes = pl.ds(pl.multiple_of((1 - odd_column) * (HALO + tile), 128), HALO)
    far_lanes = pl.ds(pl.multiple_of(odd_column * (HALO + tile), 128), HALO)
    for part in range(2):
        field_ref[part, :tall, near_lanes] = near_ref[part, :tall, :].astype(F32)
        field_ref[part, :tall, HALO : HALO + tile] = middle_ref[part].astype(F32)
        field_ref[part, :tall, far_lanes] = jnp.where(alone, 0.0, far_ref[part].astype(F32))
        field_ref[part, tall:, :] = jnp.zeros((8, wide + 128), F32)
        field_ref[part, :, wide:] = jnp.zeros((tall + 8, 128), F32)

    across_count = offset_ref.shape[2]

    def corner(number):
        i, j = divmod(number, across_count)
        return tuple(offset_ref[axis, i, j] + (JITTER + (i, j)[axis] * STEP) for axis in range(2))

    lane = lax.broadcasted_iota(jnp.int32, (1, 128), 1)
    sub = lax.broadcasted_iota(jnp.int32, (1, 8, 1), 1)
    wide_load = PROBE + 128

    def windows(number):
        top, left = corner(number)
        down, across = lax.rem(top, 8), lax.rem(left, 128)
        lanes = pl.ds(pl.multiple_of(left - across, 128), wide_load)

        def turned(part, start, height):
            rows = pl.ds(pl.multiple_of(top - down + start, 8), height)
            block = field_ref[part, rows, lanes]
            turns = [
                pltpu.roll(block[:, k : k + 128], lax.rem(128 - across, 128), 1)
                for k in range(0, wide_load, 128)
            ]
            block = jnp.concatenate(
                [jnp.where(lane < 128 - across, low, high) for low, high in zip(turns, turns[1:])], axis=1
            )
            return pltpu.roll(block.reshape(height // 8, 8, PROBE), lax.rem(8 - down, 8), 1)

        held = [turned(part, 0, 8) for part in range(2)]
        for start in range(0, PROBE, CHUNK):
            pieces = []
            for part in range(2):
                block = jnp.concatenate([held[part], turned(part, start + 8, CHUNK)], axis=0)
                pieces.append(jnp.where(sub < 8 - down, block[:-1], block[1:]).reshape(CHUNK, PROBE))
                held[part] = block[-1:]
            yield slice(start, start + CHUNK), pieces

    def add_windows(number, field):
        top, left = corner(number)
        down, across = lax.rem(top, 8), lax.rem(left, 128)
        lanes = pl.ds(pl.multiple_of(left - across, 128), wide_load)

        def add(part, start, block):
            rows = pl.ds(pl.multiple_of(top - down + start, 8), block.shape[0])
            turns = [pltpu.roll(block[:, k : k + 128], across, 1) for k in range(0, PROBE, 128)]
            empty = jnp.zeros_like(turns[0])
            block = jnp.concatenate(
                [jnp.where(lane >= across, high, low) for low, high in zip([empty, *turns], [*turns, empty])],
                axis=1,
            )
            total_ref[part, rows, lanes] = total_ref[part, rows, lanes] + block

        held = [jnp.zeros((1, 8, PROBE), F32) for _ in range(2)]
        for start in range(0, PROBE, CHUNK):
            rows = slice(start, start + CHUNK)
            real, imag = field[rows], field[PROBE + start : PROBE + start + CHUNK]
            terms = (
                probe_ref[0, rows] * real + probe_ref[1, rows] * imag,
                probe_ref[0, rows] * imag - probe_ref[1, rows] * real,
            )
            for part in range(2):
                block = pltpu.roll(terms[part].reshape(CHUNK // 8, 8, PROBE), down, 1)
                block = jnp.concatenate([held[part], block], axis=0)
                held[part] = block[-1:]
                add(part, start, jnp.where(sub >= down, block[1:], block[:-1]).reshape(CHUNK, PROBE))
        for part in range(2):
            add(part, PROBE, jnp.where(sub >= down, 0.0, held[part]).reshape(8, PROBE))

    for number in range(count):
        for rows, (real, imag) in windows(number):
            joined_ref[number, rows, :PROBE] = (
                probe_ref[0, rows] * real - probe_ref[1, rows] * imag
            ).astype(BF16)
            joined_ref[number, rows, PROBE:] = (
                probe_ref[0, rows] * imag + probe_ref[1, rows] * real
            ).astype(BF16)
    for number in range(count):
        half = jnp.dot(joined_ref[number], forward_ref[...], preferred_element_type=F32)
        stacked_ref[number, :PROBE, :] = half[:, :PROBE].astype(BF16)
        stacked_ref[number, PROBE:, :] = half[:, PROBE:].astype(BF16)
    total_ref[...] = jnp.zeros_like(total_ref)
    for number in range(count):
        wave = jnp.dot(backward_ref[...], stacked_ref[number], preferred_element_type=F32)
        real, imag = wave[:PROBE], wave[PROBE:]
        power = jnp.maximum(real * real + imag * imag, MAGNITUDE_FLOOR * MAGNITUDE_FLOOR)
        retained = 1.0 - measured_ref[number] * lax.rsqrt(power)
        joined_ref[number, :, :PROBE] = (real * retained).astype(BF16)
        joined_ref[number, :, PROBE:] = (imag * retained).astype(BF16)
    for number in range(count):
        back = jnp.dot(joined_ref[number], backward_ref[...], preferred_element_type=F32)
        stacked_ref[number, :PROBE, :] = back[:, :PROBE].astype(BF16)
        stacked_ref[number, PROBE:, :] = back[:, PROBE:].astype(BF16)
    for number in range(count):
        field = jnp.dot(forward_ref[...], stacked_ref[number], preferred_element_type=F32)
        add_windows(number, field)
    first_rows = pl.ds(pl.multiple_of((1 - odd_row) * (tall - HALO), 8), HALO)
    second_rows = pl.ds(pl.multiple_of(odd_row * (tall - HALO), 8), HALO)
    for part in range(2):
        first_ref[part] = total_ref[part, first_rows, :wide].astype(BF16)
        second_ref[part] = total_ref[part, second_rows, :wide].astype(BF16)
        own_ref[part] = total_ref[part, HALO : tall - HALO, :wide]


def gradient_terms(offsets, middle, near, far, measured, probe_field):
    tall = middle.shape[1]
    wide = middle.shape[2] + 2 * HALO
    count = measured.shape[0]
    forward, backward = dft_blocks()
    return pl.pallas_call(
        gradient_kernel,
        out_shape=(
            jax.ShapeDtypeStruct((2, HALO, wide), BF16),
            jax.ShapeDtypeStruct((2, HALO, wide), BF16),
            jax.ShapeDtypeStruct((2, tall - 2 * HALO, wide), F32),
        ),
        in_specs=[SMEM] + [VMEM] * 7,
        out_specs=(VMEM,) * 3,
        scratch_shapes=[
            pltpu.VMEM((2, tall + 8, wide + 128), F32),
            pltpu.VMEM((2, tall + 8, wide + 128), F32),
            pltpu.VMEM((count, PROBE, 2 * PROBE), BF16),
            pltpu.VMEM((count, 2 * PROBE, PROBE), BF16),
        ],
        compiler_params=params(),
        cost_estimate=pl.CostEstimate(flops=5 * 10**9, bytes_accessed=4 * 10**6, transcendentals=0),
        name="gradient",
    )(offsets, middle, near, far, measured, probe_field, forward, backward)


DATA_GRADIENT = -2.0 * DATA_STEP * RELAXATION * (2.0 * DATA_WEIGHT - 1.0)
DATA_PRIOR = 2.0 * RELAXATION * (1.0 - DATA_WEIGHT)
PRIOR_DATA = 2.0 * RELAXATION * DATA_WEIGHT
PRIOR_PRIOR = RELAXATION * (1.0 - 2.0 * DATA_WEIGHT)


def can_touch(distance):
    return distance & (distance + 1) == 0


def parcel_rows(strip, wide, tile, distance):
    return 2 * strip * (wide // 128) + 2 * strip + (2 * tile if can_touch(distance) else 0)


def strip_terms(tile_ref, data_ref, part, owner, strip):
    start = pl.multiple_of(owner * strip, strip)
    terms = (PRIOR_DATA * -2.0 * DATA_STEP) * tile_ref[part, pl.ds(start, strip), :]
    data = PRIOR_DATA * data_ref[part, pl.ds(start, strip), :]
    pieces = [terms[:, k : k + 128] for k in range(0, terms.shape[1], 128)]
    pieces[HALO // 128] = pieces[HALO // 128] + data
    return pieces


def parcel_kernel(own_ref, first_ref, second_ref, data_ref, prior_ref, tile_ref, *parcels):
    strip = prior_ref.shape[1]
    tile = data_ref.shape[2]
    row, row_count, column, _ = tile_place()
    end = (row == 0) | (row == row_count - 1)
    for part in range(2):
        value = own_ref[part] + first_ref[part].astype(F32)
        tile_ref[part] = value + jnp.where(end, 0.0, second_ref[part].astype(F32))
    for distance, parcel in enumerate(parcels, 1):
        owner = column ^ distance
        row = 0
        for part in range(2):
            for terms in strip_terms(tile_ref, data_ref, part, owner, strip):
                parcel[row : row + strip, :] = terms.astype(BF16)
                row += strip
        for part in range(2):
            lanes = pl.ds(pl.multiple_of(owner * tile, tile), tile)
            parcel[row : row + strip, :] = (DATA_PRIOR * prior_ref[part, :, lanes]).astype(BF16)
            row += strip
        if can_touch(distance):
            lanes = pl.ds(pl.multiple_of(jnp.where(owner > column, HALO + tile, 0), 128), HALO)
            for part in range(2):
                parcel[row : row + tile, :] = (DATA_GRADIENT * tile_ref[part, :, lanes]).astype(BF16)
                row += tile


def parcels_of(own, first, second, data_state, prior_reflect, columns):
    strip = prior_reflect.shape[1]
    _, tile, wide = own.shape
    shapes = [jax.ShapeDtypeStruct((2, tile, wide), F32)]
    for distance in range(1, columns):
        shapes.append(jax.ShapeDtypeStruct((parcel_rows(strip, wide, tile, distance), 128), BF16))
    return pl.pallas_call(
        parcel_kernel,
        out_shape=tuple(shapes),
        in_specs=[VMEM] * 5,
        out_specs=(VMEM,) * len(shapes),
        compiler_params=params(),
        cost_estimate=pl.CostEstimate(flops=10**8, bytes_accessed=3 * 10**6, transcendentals=0),
        name="parcels",
    )(own, first, second, data_state, prior_reflect)


def base_kernel(tile_ref, data_ref, state_ref, prior_ref, data_out, prior_out):
    strip = state_ref.shape[1]
    tile = data_ref.shape[2]
    column = lax.axis_index("col")
    own_rows = pl.ds(pl.multiple_of(column * strip, strip), strip)
    own_lanes = pl.ds(pl.multiple_of(column * tile, tile), tile)
    for part in range(2):
        data_out[part] = (
            (1.0 - RELAXATION) + RELAXATION * (2.0 * DATA_WEIGHT - 1.0)
        ) * data_ref[part] + DATA_GRADIENT * tile_ref[part, :, HALO : HALO + tile]
        data_out[part, own_rows, :] = data_out[part, own_rows, :] + DATA_PRIOR * prior_ref[part, :, own_lanes]
        width = state_ref.shape[2]
        inner = slice(HALO, HALO + width)
        prior_out[part, :, :HALO] = jnp.zeros((strip, HALO), F32)
        prior_out[part, :, HALO + width :] = jnp.zeros((strip, HALO), F32)
        prior_out[part, :, inner] = (1.0 - RELAXATION) * state_ref[part] + PRIOR_PRIOR * prior_ref[part]
        for k, terms in enumerate(strip_terms(tile_ref, data_ref, part, column, strip)):
            lanes = pl.ds(pl.multiple_of(column * tile + k * 128, 128), 128)
            prior_out[part, :, lanes] = prior_out[part, :, lanes] + terms


def own_terms(gradient, data_state, prior_state, prior_reflect):
    _, strip, width = prior_state.shape
    return pl.pallas_call(
        base_kernel,
        out_shape=(
            jax.ShapeDtypeStruct(data_state.shape, F32),
            jax.ShapeDtypeStruct((2, strip, width + 2 * HALO), F32),
        ),
        in_specs=[VMEM] * 4,
        out_specs=(VMEM,) * 2,
        compiler_params=params(),
        cost_estimate=pl.CostEstimate(flops=10**9, bytes_accessed=3 * 10**6, transcendentals=0),
        name="base",
    )(gradient, data_state, prior_state, prior_reflect)


def update_kernel(data_base, prior_base, *rest):
    *parcels, data_out, prior_out, data_ref, prior_ref, padded_ref, sems = rest
    strip, width = prior_ref.shape[1], prior_ref.shape[2]
    tile = data_ref.shape[2]
    column = lax.axis_index("col")
    blocks = 2 * HALO // 128 + tile // 128
    data_ref[...] = data_base[...]
    padded_ref[...] = prior_base[...]
    for distance, parcel in enumerate(parcels, 1):
        origin = column ^ distance
        row = 0
        for part in range(2):
            for k in range(blocks):
                lanes = pl.ds(pl.multiple_of(origin * tile + k * 128, 128), 128)
                terms = parcel[row : row + strip, :].astype(F32)
                padded_ref[part, :, lanes] = padded_ref[part, :, lanes] + terms
                row += strip
    prior_ref[...] = padded_ref[:, :, HALO : HALO + width]
    copy_prior = pltpu.make_async_copy(prior_ref, prior_out, sems.at[0])
    copy_prior.start()
    for distance, parcel in enumerate(parcels, 1):
        origin = column ^ distance
        row = 2 * strip * blocks
        rows = pl.ds(pl.multiple_of(origin * strip, strip), strip)
        for part in range(2):
            data_ref[part, rows, :] = data_ref[part, rows, :] + parcel[row : row + strip, :].astype(F32)
            row += strip
        if can_touch(distance):
            touching = (origin == column + 1) | (origin == column - 1)
            for part in range(2):
                terms = parcel[row : row + tile, :].astype(F32)
                data_ref[part] = data_ref[part] + jnp.where(touching, terms, 0.0)
                row += tile
    copy_data = pltpu.make_async_copy(data_ref, data_out, sems.at[1])
    copy_data.start()
    copy_prior.wait()
    copy_data.wait()


def new_states(data_base, prior_base, parcels):
    _, strip, padded = prior_base.shape
    width = padded - 2 * HALO
    return pl.pallas_call(
        update_kernel,
        out_shape=(
            jax.ShapeDtypeStruct(data_base.shape, F32),
            jax.ShapeDtypeStruct((2, strip, width), F32),
        ),
        in_specs=[VMEM] * (2 + len(parcels)),
        out_specs=(pl.BlockSpec(memory_space=pl.ANY),) * 2,
        scratch_shapes=[
            pltpu.VMEM(data_base.shape, F32),
            pltpu.VMEM((2, strip, width), F32),
            pltpu.VMEM(prior_base.shape, F32),
            pltpu.SemaphoreType.DMA((2,)),
        ],
        compiler_params=params(),
        cost_estimate=pl.CostEstimate(flops=10**8, bytes_accessed=3 * 10**6, transcendentals=0),
        name="update",
    )(data_base, prior_base, *parcels)


def on_device(
    probe_field,
    offsets,
    amplitudes,
    data_state,
    prior_state,
    first_weights,
    middle_weights,
    last_weights,
):
    strip = prior_state.shape[1]
    columns = lax.axis_size("col")

    small = packed(data_state, prior_state)
    first = swap(small, ROWS, 0, True)
    second = swap(small, ROWS, 1, True)
    middle_near, middle, edge = widened(small, first, second, prior_state)
    near = swap(middle_near, "col", 0, False)
    far = swap(middle, "col", 1, False)
    edge = swap(edge, "col", 1, True)
    weights, _ = lax.optimization_barrier(((first_weights, middle_weights, last_weights), middle))
    bands = banded_weights(strip, *weights)
    first, second, own = gradient_terms(
        offsets, middle, near, far, amplitudes.reshape(-1, PROBE, PROBE), probe_field
    )
    first = swap(first, ROWS, 0, True)
    second = swap(second, ROWS, 1, True)
    reflect = prior_reflection(prior_state, near, edge, bands)
    gradient, *parcels = parcels_of(own, first, second, data_state, reflect, columns)
    bases = own_terms(gradient, data_state, prior_state, reflect)
    received = []
    for distance, parcel in enumerate(parcels, 1):
        received.append(cross(parcel, "col", distance))
    return new_states(*bases, received)


def solution(mesh):
    placed = (
        P(),
        P(None, ROWS, "col"),
        P(ROWS, "col", None, None),
        P(None, ROWS, "col"),
        P(None, STRIPS, None),
        P(),
        P(),
        P(),
    )
    return jax.shard_map(
        on_device,
        mesh=mesh,
        in_specs=placed,
        out_specs=(P(None, ROWS, "col"), P(None, STRIPS, None)),
        check_vma=False,
    )
```
